512 devices in a mesh: flow: 128 (over z, x, core), leaf: 4 (over y).
Axes of the slice: x: 4, y: 4, z: 16, core: 2. Of those that a mesh axis runs over, the one named last changes fastest.
Arguments:
- vel_coef: float32 [81, 262144], P(None, 'flow'), may hold values from -6 to 6
- gp_block: int32 [1048576, 1], P(('flow', 'leaf')), may hold values from 0 to 127; in each aligned block of 2048 rows (0 to 2047, 2048 to 4095, ...) at most 32 rows name the same one
- gp_elem: int32 [1048576], P(('flow', 'leaf')), may hold values from 0 to 2047
- gp_param: float32 [3, 1048576], P(None, ('flow', 'leaf')), may hold values from 0 to 1
- gp_vel: float32 [3, 1048576], P(None, ('flow', 'leaf')), may hold values from -6 to 6
- gp_weight: float32 [1048576], P(('flow', 'leaf')), may hold values from 0.1 to 1
- gp_pos: float32 [3, 1048576], P(None, ('flow', 'leaf')), may hold values from -4 to 4
- contact_patch: int32 [1048576], P(('flow', 'leaf')), may hold values from 0 to 1023
- contact_param: float32 [2, 1048576], P(None, ('flow', 'leaf')), may hold values from 0 to 1
- patch_ctrl: float32 [27, 131072], P(None, ('flow', 'leaf')), may hold values from -4 to 4
Outputs:
- flow_force: float32 [81, 262144], P(None, ('flow', 'leaf'))
- shell_force: float32 [3, 1048576], P(None, ('flow', 'leaf'))
- patch_force: float32 [27, 131072], P(None, ('flow', 'leaf'))
The draws below stay inside these ranges and needn't reach their ends.
Inputs may be any that keep to these rules, and one draw needn't show every extreme that they name: `gp_block`: the Gauss points of one device lie in at most 32 of each flow block's elements; some block is reached with exactly 32. `contact_patch`: A contact partner is one of the 1024 patches held by the Gauss point's own group, the devices of one index of flow.
All inputs are finite; a program needn't handle non-finite values.
Results may differ from the reference program's by a relative error of at most 0.0001.
Values sent between devices are 32-bit elements; how exact they have to be, the bound alone decides.
A program may use at most 64 MiB of HBM per device.

```python
import math
import jax
import jax.numpy as jnp
import numpy as np

E_DEV = 2048
GP_DEV = 2048
CAP = 32
NELEM = 262144
GP = 1048576
NP_GROUP = 1024
NPATCH = 131072
N_FLOW = 128
N_LEAF = 4


def with_ends(array, stream_key, least, high):
    extent = array.shape
    spot = [jax.random.randint(jax.random.fold_in(stream_key, axis), (), 0, extent[axis]) for axis in range(len(extent))]
    array = array.at[tuple(spot)].set(least)
    longest = extent.index(max(extent))
    spot[longest] = (spot[longest] + 1) % extent[longest]
    return array.at[tuple(spot)].set(high)


def level_of(key, extent, pieces, low, largest):
    def one(dim, shards_of):
        steps = jax.random.uniform(jax.random.fold_in(jax.random.fold_in(key, 6), dim), (shards_of,), jnp.float32, low / len(pieces), largest / len(pieces))
        return jnp.repeat(jnp.exp(steps), extent[dim] // shards_of).reshape((-1,) + (1,) * (len(extent) - dim - 1))

    gain = one(*pieces[0])
    for cut in pieces[1:]:
        gain = gain * one(*cut)
    return gain


def shared_out(key, own, number, rows, amount, top, reach, skew):
    ranking = jax.random.permutation(key, amount)
    packed, usual = shares(amount, rows * top, reach, skew, True), shares(amount, rows * top, reach, skew, False)
    places = jnp.arange(amount)

    def named(lengths, offset_by):
        used = int((lengths > 0).sum())
        fixed = max(1, used // 4)
        moved = fixed + (places - fixed + offset_by * (used - fixed)) % max(1, amount - fixed)
        return jnp.zeros((amount,), jnp.int32).at[ranking[jnp.where(places < fixed, places, moved)]].set(jnp.asarray(lengths, jnp.int32))

    lengths = jnp.where(number % 4 == 0, named(packed, number // 4), named(usual, number - number // 4 - 1))
    mixed = jax.random.permutation(jax.random.fold_in(own, 3), amount)
    source_of, receiver = mixed[0:amount // 2 * 2:2], mixed[1:amount // 2 * 2:2]
    room = jnp.minimum(lengths[source_of] - 1, reach - lengths[receiver]) // 2
    room = jnp.where((source_of == ranking[0]) | (receiver == ranking[0]) | (lengths[receiver] == 0), 0, jnp.maximum(room, 0))
    moved = jax.random.randint(jax.random.fold_in(own, 4), (amount // 2,), 0, 1 << 20) % (room + 1)
    lengths = lengths.at[source_of].add(-moved).at[receiver].add(moved)
    labels = jnp.searchsorted(jnp.cumsum(lengths), jnp.arange(rows * top), side="right").astype(jnp.int32)
    table = labels.reshape(top, rows).T
    table = table[jax.random.permutation(jax.random.fold_in(own, 1), rows)]
    offset_by = jax.random.randint(jax.random.fold_in(own, 2), (rows, 1), 0, top)
    return jnp.take_along_axis(table, (jnp.arange(top)[None, :] + offset_by) % top, axis=1)


def shares(number_of, total, limit, skew, full):
    portions = [(1 << 20) // math.isqrt(standing ** skew) + 1 for standing in range(1, number_of + 1)]
    largest = limit if full else min(limit, max(-(-total // number_of), total * portions[0] // sum(portions)))
    least = 1 if total - largest >= number_of - 1 else 0
    holding, spare = [largest] + [least] * (number_of - 1), total - largest - least * (number_of - 1)
    while spare > 0:
        candidates = [i for i in range(1, number_of) if holding[i] < largest] or [i for i in range(1, number_of) if holding[i] < limit]
        pool, left = sum([portions[i] for i in candidates]), spare
        for i in candidates:
            addition = min(limit - holding[i], max(1, left * portions[i] // pool), spare)
            holding[i] = holding[i] + addition
            spare = spare - addition
    return np.array(holding)


def centred(stream_key, shape, deviation, most, shards=(), kind=jnp.bfloat16):
    array = deviation * jax.random.normal(stream_key, shape, jnp.float32)
    if shards:
        array = array * level_of(stream_key, shape, shards, -0.22, 0.18)
    return jnp.clip(array, -most, most).astype(kind)


def setup_inputs(seed: int = 0) -> dict:
    key_of = jax.random.split(jax.random.key(seed), 11)
    vel_coef = centred(key_of[0], (81, NELEM), 1.0, 6.0, ((1, 128),), jnp.float32)
    gp_block_keys = jax.random.split(jax.random.fold_in(key_of[1], 1), GP // GP_DEV)
    gp_block_turns = jax.random.permutation(jax.random.fold_in(key_of[1], 3), GP // GP_DEV)
    gp_block = jax.vmap(lambda own, number: shared_out(jax.random.fold_in(key_of[1], 2), own, number, GP_DEV, N_FLOW, 1, CAP, 2))(gp_block_keys, gp_block_turns).reshape((GP, 1))
    gp_elem = with_ends(jax.random.randint(key_of[2], (GP,), 0, E_DEV), jax.random.fold_in(key_of[2], 1), 0, E_DEV - 1).astype(jnp.int32)
    gp_param = jnp.clip(1.0 * jax.random.uniform(key_of[3], (3, GP), jnp.float32) ** level_of(key_of[3], (3, GP), ((1, 512),), -0.2, 0.2), 0.0, 1.0)
    gp_vel = centred(key_of[4], (3, GP), 1.0, 6.0, ((1, 512),), jnp.float32)
    gp_weight = jnp.clip(jnp.exp(math.log(1.0) - 2.3025851 * jax.random.uniform(key_of[5], (GP,), jnp.float32) ** level_of(key_of[5], (GP,), ((0, 512),), -0.2, 0.2)), 0.1, 1.0)
    gp_pos = centred(key_of[6], (3, GP), 0.5, 4.0, ((1, 512),), jnp.float32)
    contact_patch = with_ends(jax.random.randint(key_of[7], (GP,), 0, NP_GROUP), jax.random.fold_in(key_of[7], 1), 0, NP_GROUP - 1).astype(jnp.int32)
    contact_param = jnp.clip(1.0 * jax.random.uniform(key_of[8], (2, GP), jnp.float32) ** level_of(key_of[8], (2, GP), ((1, 512),), -0.2, 0.2), 0.0, 1.0)
    patch_ctrl = centred(key_of[9], (27, NPATCH), 0.5, 4.0, ((1, 512),), jnp.float32)
    return dict(vel_coef=vel_coef, gp_block=gp_block, gp_elem=gp_elem, gp_param=gp_param, gp_vel=gp_vel, gp_weight=gp_weight, gp_pos=gp_pos, contact_patch=contact_patch, contact_param=contact_param, patch_ctrl=patch_ctrl)


BETA = 1.5
STIFF = 2.0
REACH = 0.5


def basis(x):
    return jnp.stack([0.5 * (1.0 - x) ** 2, 0.5 * (1.0 + 2.0 * x - 2.0 * x * x), 0.5 * x * x])


def solid_weights(param):
    first, second, third = basis(param[0]), basis(param[1]), basis(param[2])
    return (first[:, None, None, :] * second[None, :, None, :] * third[None, None, :, :]).reshape(27, -1)


def shell_weights(param):
    first, second = basis(param[0]), basis(param[1])
    return (first[:, None, :] * second[None, :, :]).reshape(9, -1)


def contact_force(position, partner_coef, weights):
    near = jnp.sum(partner_coef.reshape(3, 9, -1) * weights[None], axis=1)
    gap = position - near
    return STIFF * gap / (1.0 + jnp.sum(gap * gap, axis=0) / (REACH * REACH))


def reference(vel_coef, gp_block, gp_elem, gp_param, gp_vel, gp_weight, gp_pos, contact_patch, contact_param, patch_ctrl):
    gelem = (gp_block[:, 0] * E_DEV + gp_elem).astype(jnp.int32)
    weights = solid_weights(gp_param)
    speeds = []
    for comp in range(3):
        speeds.append(jnp.sum(vel_coef[comp * 27:(comp + 1) * 27][:, gelem] * weights, axis=0))
    speed = jnp.stack(speeds)
    fsi = BETA * gp_weight[None, :] * (gp_vel - speed)
    rows = []
    for comp in range(3):
        part_rows = jnp.zeros((27, NELEM), vel_coef.dtype).at[:, gelem].add(weights * fsi[comp][None, :])
        rows.append(part_rows)
    flow_force = jnp.concatenate(rows, axis=0)
    points = jnp.arange(GP, dtype=jnp.int32)
    partner = ((points // (GP_DEV * N_LEAF)) * NP_GROUP + contact_patch).astype(jnp.int32)
    shell_w = shell_weights(contact_param)
    pushes = contact_force(gp_pos, patch_ctrl[:, partner], shell_w)
    reaction = -(pushes[:, None, :] * shell_w[None]).reshape(27, -1)
    patch_force = jnp.zeros((27, NPATCH), patch_ctrl.dtype).at[:, partner].add(reaction)
    shell_force = pushes - fsi
    return flow_force, shell_force, patch_force
```

```python
import functools

import jax
import jax.numpy as jnp
from jax import lax
from jax.experimental import pallas as pl
from jax.experimental.pallas import tpu as pltpu
from jax.sharding import PartitionSpec as P

BETA = 1.5
STIFF = 2.0
REACH = 0.5
CAP = 32
LANES = 128
F32 = jnp.float32
BF16 = jnp.bfloat16
MESH = pl.DeviceIdType.MESH
NT = (((1,), (1,)), ((), ()))


def split(x):
    high = x.astype(BF16)
    return high, (x - high.astype(F32)).astype(BF16)


def basis(x):
    return (0.5 * (1.0 - x) ** 2, 0.5 * (1.0 + 2.0 * x - 2.0 * x * x), 0.5 * x * x)


def pick(digit, values):
    return jnp.where(digit == 0, values[0], jnp.where(digit == 1, values[1], values[2]))


def one_hot(row, base, rows):
    step = min(rows, 256)
    number = lax.broadcasted_iota(jnp.int32, (step, LANES), 0).astype(F32).astype(BF16)
    one, zero = jnp.ones((step, LANES), BF16), jnp.zeros((step, LANES), BF16)
    out = []
    for first in range(0, rows, step):
        near = jnp.broadcast_to(row - float(base + first), (16, LANES)).astype(BF16)
        near = jnp.concatenate([near] * (step // 16), axis=0)
        out.append(jnp.where(number == near, one, zero))
    return jnp.concatenate(out, axis=0) if len(out) > 1 else out[0]


def kernel(
    vel_coef, dest_ref, elem_ref, param_ref, vel_ref, weight_ref, pos_ref, patch_ref, cparam_ref, ctrl_ref,
    flow_out, shell_out, patch_out,
    dest_hot, rank_row, packed, message, received, slots, coef, hot, terms, force_rows, answer, returned,
    contact_hot, contact_terms, push, ctrl_all, patch_part, patch_all, flow_part, flow_all,
    out_sem, back_sem, ctrl_sem, patch_sem, flow_sem,
):
    owners, peers = lax.axis_size("flow"), lax.axis_size("leaf")
    me, leaf = lax.axis_index("flow"), lax.axis_index("leaf")
    points = dest_ref.shape[1]
    elements = vel_coef.shape[1]
    per_leaf = elements // peers
    patches = ctrl_ref.shape[1]
    total_slots = CAP * owners

    def flow_peer(i):
        half = (i + 1) // 2
        return lax.rem(me + jnp.where(lax.rem(i, 2) == 0, owners // 2 + half, owners // 2 - half), owners)

    def leaf_peer(i):
        return lax.rem(leaf + 1 + i, peers)

    barrier = pltpu.get_barrier_semaphore()

    def greet(i, carry):
        pl.semaphore_signal(barrier, inc=1, device_id=(flow_peer(i), leaf), device_id_type=MESH)
        return carry

    lax.fori_loop(0, owners - 1, greet, 0)
    for i in range(peers - 1):
        pl.semaphore_signal(barrier, inc=1, device_id=(me, leaf_peer(i)), device_id_type=MESH)

    owner_number = lax.broadcasted_iota(jnp.int32, (owners, points), 0)
    dest_hot[...] = jnp.where(owner_number == dest_ref[...], 1.0, 0.0).astype(BF16)
    block = 256
    before = (
        lax.broadcasted_iota(jnp.int32, (block, block), 0) < lax.broadcasted_iota(jnp.int32, (block, block), 1)
    ).astype(F32).astype(BF16)
    carry = jnp.zeros((owners, 1), F32)
    for b in range(points // block):
        part = dest_hot[:, b * block : (b + 1) * block]
        ahead = jnp.dot(part, before, preferred_element_type=F32)
        wide = part.astype(F32)
        rank_row[:, b * block : (b + 1) * block] = jnp.sum(wide * (ahead + carry), axis=0, keepdims=True)
        carry = carry + jnp.sum(wide, axis=1, keepdims=True)

    rank_hot = lax.broadcasted_iota(jnp.int32, (CAP, points), 0).astype(F32) == rank_row[...]
    values = [elem_ref[...].astype(F32)]
    values += [param_ref[i : i + 1, :] for i in range(3)]
    values += [vel_ref[i : i + 1, :] for i in range(3)]
    values += [BETA * weight_ref[...]]
    for v, value in enumerate(values):
        high = value.astype(BF16).astype(F32)
        packed[v * CAP : (v + 1) * CAP, :] = jnp.where(rank_hot, high, 0.0).astype(BF16)
        packed[(8 + v) * CAP : (9 + v) * CAP, :] = jnp.where(rank_hot, value - high, 0.0).astype(BF16)
    spread = lax.dot_general(packed[...], dest_hot[...], NT, preferred_element_type=F32)
    spread = spread[: 8 * CAP] + spread[8 * CAP :]
    for h in range(2):
        message[pl.ds(h, owners, stride=2), :] = jnp.transpose(spread[h * LANES : (h + 1) * LANES])

    pl.semaphore_wait(barrier, owners - 1 + peers - 1)

    def out_copy(peer):
        return pltpu.make_async_remote_copy(
            src_ref=message.at[pl.ds(pl.multiple_of(2 * peer, 2), 2), :],
            dst_ref=received.at[pl.ds(pl.multiple_of(2 * me, 2), 2), :],
            send_sem=out_sem.at[0], recv_sem=out_sem.at[1],
            device_id=(peer, leaf), device_id_type=MESH,
        )

    def send_out(i, carry):
        out_copy(flow_peer(i)).start()
        return carry

    def ctrl_copy(peer):
        return pltpu.make_async_remote_copy(
            src_ref=ctrl_ref, dst_ref=ctrl_all.at[leaf], send_sem=ctrl_sem.at[0], recv_sem=ctrl_sem.at[1],
            device_id=(me, peer), device_id_type=MESH,
        )

    for i in range(peers - 1):
        ctrl_copy(leaf_peer(i)).start()
    lax.fori_loop(0, owners - 1, send_out, 0)
    mine = pl.ds(pl.multiple_of(2 * me, 2), 2)
    received[mine, :] = message[mine, :]
    ctrl_all[leaf] = ctrl_ref[...]

    coef[...] = jnp.zeros_like(coef)
    for c in range(3):
        high, low = split(vel_coef[c * 27 : (c + 1) * 27, :])
        coef[c * 32 : c * 32 + 27, :] = high
        coef[96 + c * 32 : 96 + c * 32 + 27, :] = low

    pltpu.make_async_remote_copy(
        src_ref=ctrl_all.at[: peers - 1], dst_ref=ctrl_all.at[: peers - 1], send_sem=ctrl_sem.at[0],
        recv_sem=ctrl_sem.at[1], device_id=(me, leaf_peer(0)), device_id_type=MESH,
    ).wait()
    zero7 = jnp.zeros((7, peers * patches), F32)
    whole = jnp.concatenate([ctrl_all[i] for i in range(peers)], axis=1)
    whole = jnp.concatenate([part for c in range(3) for part in (whole[c * 9 : (c + 1) * 9], zero7)], axis=0)
    ctrl_high, ctrl_low = split(whole)
    ctrl_terms = jnp.concatenate([ctrl_high, ctrl_low], axis=0)
    shell_k = lax.broadcasted_iota(jnp.int32, (16, 1), 0)
    contact_terms[...] = jnp.zeros_like(contact_terms)
    wide = 512
    for j in range(points // wide):
        cols = slice(j * wide, (j + 1) * wide)
        for i in range(wide // LANES):
            at = slice(j * wide + i * LANES, j * wide + (i + 1) * LANES)
            contact_hot[:, at] = one_hot(patch_ref[:, at].astype(F32), 0, peers * patches)
        taken = jnp.dot(ctrl_terms, contact_hot[:, cols], preferred_element_type=F32)
        taken = taken[:48] + taken[48:]
        weights = pick(shell_k // 3, basis(cparam_ref[0:1, cols])) * pick(
            lax.rem(shell_k, 3), basis(cparam_ref[1:2, cols])
        )
        weights = jnp.where(shell_k < 9, weights, 0.0)
        gap = [
            pos_ref[c : c + 1, cols] - jnp.sum(taken[c * 16 : (c + 1) * 16] * weights, axis=0, keepdims=True)
            for c in range(3)
        ]
        scale = STIFF / (1.0 + (gap[0] * gap[0] + gap[1] * gap[1] + gap[2] * gap[2]) / (REACH * REACH))
        for c in range(3):
            fc = scale * gap[c]
            push[c : c + 1, cols] = fc
            high, low = split(-(weights * fc))
            contact_terms[c * 16 : (c + 1) * 16, cols] = high
            contact_terms[64 + c * 16 : 64 + (c + 1) * 16, cols] = low
    reaction = lax.dot_general(contact_hot[...], contact_terms[...], NT, preferred_element_type=F32)
    reaction = jnp.transpose(reaction)
    reaction = reaction[:48] + reaction[64:112]
    for q in range(peers):
        for c in range(3):
            patch_part[q, c * 9 : (c + 1) * 9, :] = reaction[c * 16 : c * 16 + 9, q * patches : (q + 1) * patches]

    def patch_copy(peer):
        return pltpu.make_async_remote_copy(
            src_ref=patch_part.at[peer], dst_ref=patch_all.at[leaf], send_sem=patch_sem.at[0],
            recv_sem=patch_sem.at[1], device_id=(me, peer), device_id_type=MESH,
        )

    for i in range(peers - 1):
        patch_copy(leaf_peer(i)).start()
    patch_all[leaf] = patch_part[leaf]

    pltpu.make_async_remote_copy(
        src_ref=message.at[: 2 * (owners - 1), :], dst_ref=received.at[: 2 * (owners - 1), :],
        send_sem=out_sem.at[0], recv_sem=out_sem.at[1], device_id=(flow_peer(0), leaf), device_id_type=MESH,
    ).wait()
    for h in range(2):
        rows = jnp.transpose(received[pl.ds(h, owners, stride=2), :])
        for i in range(4):
            slots[4 * h + i] = rows[i * CAP : (i + 1) * CAP]
    solid_k = lax.broadcasted_iota(jnp.int32, (32, 1), 0)
    digits = (solid_k // 9, lax.rem(solid_k // 3, 3), lax.rem(solid_k, 3))
    force_rows[...] = jnp.zeros_like(force_rows)
    terms[96:128, :] = jnp.zeros((32, total_slots), BF16)
    terms[224:256, :] = jnp.zeros((32, total_slots), BF16)
    ranks = 4

    def owner_step(j, carry):
        cols = pl.ds(pl.multiple_of(j * ranks * LANES, ranks * LANES), ranks * LANES)
        hot[:, cols] = jnp.concatenate(
            [one_hot(slots[0, pl.ds(j * ranks + i, 1), :], 0, elements) for i in range(ranks)], axis=1
        )
        taken = jnp.dot(coef[...], hot[:, cols], preferred_element_type=F32)
        taken = taken[:96] + taken[96:]
        for i in range(ranks):
            r = j * ranks + i
            row = pl.ds(r, 1)
            weights = pick(digits[0], basis(slots[1, row, :]))
            weights = weights * pick(digits[1], basis(slots[2, row, :]))
            weights = weights * pick(digits[2], basis(slots[3, row, :]))
            weights = jnp.where(solid_k < 27, weights, 0.0)
            at = pl.ds(pl.multiple_of(r * LANES, LANES), LANES)
            for c in range(3):
                speed = jnp.sum(
                    taken[c * 32 : (c + 1) * 32, i * LANES : (i + 1) * LANES] * weights, axis=0, keepdims=True
                )
                force = slots[7, row, :] * (slots[4 + c, row, :] - speed)
                force_rows[pl.ds(c * CAP + r, 1), :] = force
                high, low = split(weights * force)
                terms[c * 32 : (c + 1) * 32, at] = high
                terms[128 + c * 32 : 128 + (c + 1) * 32, at] = low
        return carry

    lax.fori_loop(0, CAP // ranks, owner_step, 0)
    answer[...] = jnp.transpose(force_rows[...])

    def back_copy(peer):
        return pltpu.make_async_remote_copy(
            src_ref=answer.at[pl.ds(peer, 1), :], dst_ref=returned.at[pl.ds(me, 1), :],
            send_sem=back_sem.at[0], recv_sem=back_sem.at[1], device_id=(peer, leaf), device_id_type=MESH,
        )

    def send_back(i, carry):
        back_copy(flow_peer(i)).start()
        return carry

    lax.fori_loop(0, owners - 1, send_back, 0)
    returned[pl.ds(me, 1), :] = answer[pl.ds(me, 1), :]

    def quarter(q):
        part = lax.dot_general(
            hot[pl.ds(pl.multiple_of(q * per_leaf, per_leaf), per_leaf), :], terms[...], NT, preferred_element_type=F32
        )
        part = jnp.transpose(part[:, :LANES] + part[:, LANES:])
        for c in range(3):
            flow_part[q, c * 27 : (c + 1) * 27, :] = part[c * 32 : c * 32 + 27]

    def flow_copy(peer):
        return pltpu.make_async_remote_copy(
            src_ref=flow_part.at[peer], dst_ref=flow_all.at[leaf], send_sem=flow_sem.at[0],
            recv_sem=flow_sem.at[1], device_id=(me, peer), device_id_type=MESH,
        )

    def spread_quarter(i, carry):
        peer = leaf_peer(i)
        quarter(peer)
        flow_copy(peer).start()
        return carry

    lax.fori_loop(0, peers - 1, spread_quarter, 0)
    quarter(leaf)
    flow_all[leaf] = flow_part[leaf]

    pltpu.make_async_remote_copy(
        src_ref=patch_part.at[: peers - 1], dst_ref=patch_all.at[: peers - 1], send_sem=patch_sem.at[0],
        recv_sem=patch_sem.at[1], device_id=(me, leaf_peer(0)), device_id_type=MESH,
    ).wait()
    patch_out[...] = (patch_all[0] + patch_all[1]) + (patch_all[2] + patch_all[3])

    pltpu.make_async_remote_copy(
        src_ref=answer.at[: owners - 1, :], dst_ref=returned.at[: owners - 1, :], send_sem=back_sem.at[0],
        recv_sem=back_sem.at[1], device_id=(flow_peer(0), leaf), device_id_type=MESH,
    ).wait()
    high, low = split(jnp.transpose(returned[...]))
    twice = jnp.concatenate([dest_hot[...], dest_hot[...]], axis=0)
    at_owner = jnp.dot(jnp.concatenate([high, low], axis=1), twice, preferred_element_type=F32)
    rank_hot = lax.broadcasted_iota(jnp.int32, (CAP, points), 0).astype(F32) == rank_row[...]
    for c in range(3):
        fsi = jnp.sum(jnp.where(rank_hot, at_owner[c * CAP : (c + 1) * CAP], 0.0), axis=0, keepdims=True)
        shell_out[c : c + 1, :] = push[c : c + 1, :] - fsi

    pltpu.make_async_remote_copy(
        src_ref=flow_part.at[: peers - 1], dst_ref=flow_all.at[: peers - 1], send_sem=flow_sem.at[0],
        recv_sem=flow_sem.at[1], device_id=(me, leaf_peer(0)), device_id_type=MESH,
    ).wait()
    flow_out[...] = (flow_all[0] + flow_all[1]) + (flow_all[2] + flow_all[3])


def solution(mesh):
    owners, peers = mesh.shape["flow"], mesh.shape["leaf"]

    def per_device(
        vel_coef, gp_block, gp_elem, gp_param, gp_vel, gp_weight, gp_pos, contact_patch, contact_param, patch_ctrl
    ):
        points, elements, patches = gp_elem.shape[0], vel_coef.shape[1], patch_ctrl.shape[1]
        total_slots = CAP * owners
        vmem = pl.BlockSpec(memory_space=pltpu.VMEM)
        return pl.pallas_call(
            kernel,
            out_shape=(
                jax.ShapeDtypeStruct((81, elements // peers), F32),
                jax.ShapeDtypeStruct((3, points), F32),
                jax.ShapeDtypeStruct((27, patches), F32),
            ),
            in_specs=[vmem] * 10,
            out_specs=(vmem,) * 3,
            scratch_shapes=[
                pltpu.VMEM((owners, points), BF16),
                pltpu.VMEM((1, points), F32),
                pltpu.VMEM((16 * CAP, points), BF16),
                pltpu.VMEM((2 * owners, LANES), F32),
                pltpu.VMEM((2 * owners, LANES), F32),
                pltpu.VMEM((8, CAP, LANES), F32),
                pltpu.VMEM((192, elements), BF16),
                pltpu.VMEM((elements, total_slots), BF16),
                pltpu.VMEM((256, total_slots), BF16),
                pltpu.VMEM((LANES, owners), F32),
                pltpu.VMEM((owners, LANES), F32),
                pltpu.VMEM((owners, LANES), F32),
                pltpu.VMEM((peers * patches, points), BF16),
                pltpu.VMEM((LANES, points), BF16),
                pltpu.VMEM((3, points), F32),
                pltpu.VMEM((peers, 27, patches), F32),
                pltpu.VMEM((peers, 27, patches), F32),
                pltpu.VMEM((peers, 27, patches), F32),
                pltpu.VMEM((peers, 81, elements // peers), F32),
                pltpu.VMEM((peers, 81, elements // peers), F32),
                pltpu.SemaphoreType.DMA((2,)),
                pltpu.SemaphoreType.DMA((2,)),
                pltpu.SemaphoreType.DMA((2,)),
                pltpu.SemaphoreType.DMA((2,)),
                pltpu.SemaphoreType.DMA((2,)),
            ],
            compiler_params=pltpu.CompilerParams(
                collective_id=0, has_side_effects=True, vmem_limit_bytes=60 * 1024 * 1024
            ),
        )(
            vel_coef,
            gp_block.reshape(1, points),
            gp_elem.reshape(1, points),
            gp_param,
            gp_vel,
            gp_weight.reshape(1, points),
            gp_pos,
            contact_patch.reshape(1, points),
            contact_param,
            patch_ctrl,
        )

    both = ("flow", "leaf")
    return jax.shard_map(
        per_device,
        mesh=mesh,
        in_specs=(
            P(None, "flow"), P(both, None), P(both), P(None, both), P(None, both),
            P(both), P(None, both), P(both), P(None, both), P(None, both),
        ),
        out_specs=(P(None, both), P(None, both), P(None, both)),
        check_vma=False,
    )
```

```python
import jax
import jax.numpy as jnp
from jax import lax
from jax.experimental import pallas as pl
from jax.experimental.pallas import tpu as pltpu
from jax.sharding import PartitionSpec as P

BETA = 1.5
STIFF = 2.0
REACH = 0.5
CAP = 32
LANES = 128
GROUPS = 4
HALF = 96
PITCH = 104
F32 = jnp.float32
BF16 = jnp.bfloat16
MESH = pl.DeviceIdType.MESH
NT = (((1,), (1,)), ((), ()))


def split(x):
    high = x.astype(BF16)
    return high, (x - high.astype(F32)).astype(BF16)


def basis(x):
    return (0.5 * (1.0 - x) ** 2, 0.5 * (1.0 + 2.0 * x - 2.0 * x * x), 0.5 * x * x)


def pick(digit, values):
    return jnp.where(digit == 0, values[0], jnp.where(digit == 1, values[1], values[2]))


def one_hot(row, rows):
    step = min(rows, 256)
    number = lax.broadcasted_iota(jnp.int32, (step, LANES), 0).astype(F32).astype(BF16)
    one, zero = jnp.ones((step, LANES), BF16), jnp.zeros((step, LANES), BF16)
    out = []
    for first in range(0, rows, step):
        near = jnp.broadcast_to(row - float(first), (16, LANES)).astype(BF16)
        near = jnp.concatenate([near] * (step // 16), axis=0)
        out.append(jnp.where(number == near, one, zero))
    return jnp.concatenate(out, axis=0) if len(out) > 1 else out[0]


def kernel(
    vel_coef_hbm, dest_hbm, elem_hbm, param_hbm, vel_hbm, weight_hbm, pos_hbm, patch_hbm, cparam_hbm, ctrl_hbm,
    flow_out, shell_out, patch_out,
    vel_coef, dest_ref, elem_ref, param_ref, vel_ref, weight_ref, pos_ref, patch_ref, cparam_ref, ctrl_ref,
    dest_hot, rank_row, packed, message, received, places, coef, forces, turned, flipped, answer, returned,
    strided, total, contact_terms, push, ctrl_all, patch_part, patch_all,
    in_sem, out_send, out_recv, back_sem, ctrl_sem, patch_sem, place_send, place_recv, force_send, force_recv,
):
    owners, peers = lax.axis_size("flow"), lax.axis_size("leaf")
    me, leaf = lax.axis_index("flow"), lax.axis_index("leaf")
    points = dest_ref.shape[1]
    elements = vel_coef.shape[1]
    per_leaf = elements // peers
    patches = ctrl_ref.shape[1]
    members = owners // GROUPS
    ranks = CAP * members // LANES

    def offset(position):
        return (position + 1) // 2 if position % 2 else (owners - position // 2) % owners

    def ahead_of(position):
        return lax.rem(me + offset(position), owners)

    def behind(position):
        return lax.rem(me + (owners - offset(position)), owners)

    def leaf_peer(i):
        return lax.rem(leaf + i, peers)

    inputs = [
        (dest_hbm, dest_ref), (elem_hbm, elem_ref), (param_hbm, param_ref), (vel_hbm, vel_ref),
        (weight_hbm, weight_ref), (ctrl_hbm, ctrl_ref), (patch_hbm, patch_ref), (pos_hbm, pos_ref),
        (cparam_hbm, cparam_ref), (vel_coef_hbm, vel_coef),
    ]
    fetches = [pltpu.make_async_copy(src, dst, in_sem.at[i]) for i, (src, dst) in enumerate(inputs)]
    for fetch in fetches:
        fetch.start()
    barrier = pltpu.get_barrier_semaphore()
    for position in range(owners - 1, 0, -1):
        pl.semaphore_signal(barrier, inc=1, device_id=(behind(position), leaf), device_id_type=MESH)
    for i in range(1, peers):
        pl.semaphore_signal(barrier, inc=1, device_id=(me, leaf_peer(i)), device_id_type=MESH)

    for fetch in fetches[:6]:
        fetch.wait()
    position = lax.broadcasted_iota(jnp.int32, (owners, 1), 0)
    distance = jnp.where(
        lax.rem(position, 2) == 1, (position + 1) // 2, jnp.where(position == 0, 0, owners - position // 2)
    )
    away = dest_ref[...] - me
    away = jnp.where(away < 0, away + owners, away)
    dest_hot[...] = jnp.where(distance == away, 1.0, 0.0).astype(BF16)
    block = 256
    before = (
        lax.broadcasted_iota(jnp.int32, (block, block), 0) < lax.broadcasted_iota(jnp.int32, (block, block), 1)
    ).astype(F32).astype(BF16)
    carry = jnp.zeros((owners, 1), F32)
    for b in range(points // block):
        part = dest_hot[:, b * block : (b + 1) * block]
        earlier = jnp.dot(part, before, preferred_element_type=F32)
        wide = part.astype(F32)
        rank_row[:, b * block : (b + 1) * block] = jnp.sum(wide * (earlier + carry), axis=0, keepdims=True)
        carry = carry + jnp.sum(wide, axis=1, keepdims=True)

    rank_hot = lax.broadcasted_iota(jnp.int32, (CAP, points), 0).astype(F32) == rank_row[...]
    values = [elem_ref[...].astype(F32)]
    values += [param_ref[i : i + 1, :] for i in range(3)]
    values += [vel_ref[i : i + 1, :] for i in range(3)]
    values += [BETA * weight_ref[...]]
    for v, value in enumerate(values):
        high = value.astype(BF16).astype(F32)
        for h in range(2):
            chosen = rank_hot[h * 16 : (h + 1) * 16]
            at = h * LANES + v * 16
            packed[at : at + 16, :] = jnp.where(chosen, high, 0.0).astype(BF16)
            packed[2 * LANES + at : 2 * LANES + at + 16, :] = jnp.where(chosen, value - high, 0.0).astype(BF16)
    spread = lax.dot_general(packed[...], dest_hot[...], NT, preferred_element_type=F32)
    spread = spread[: 2 * LANES] + spread[2 * LANES :]
    for h in range(2):
        message[pl.ds(h, owners, stride=2), :] = jnp.transpose(spread[h * LANES : (h + 1) * LANES])

    pl.semaphore_wait(barrier, owners - 1 + peers - 1)

    ctrl_copies = [
        pltpu.make_async_remote_copy(
            src_ref=ctrl_ref, dst_ref=ctrl_all.at[leaf], send_sem=ctrl_sem.at[0], recv_sem=ctrl_sem.at[1],
            device_id=(me, leaf_peer(i)), device_id_type=MESH,
        )
        for i in range(1, peers)
    ]
    for copy in ctrl_copies:
        copy.start()
    for position in range(1, owners):
        rows = pl.ds(2 * position, 2)
        pltpu.make_async_remote_copy(
            src_ref=message.at[rows, :], dst_ref=received.at[rows, :], send_sem=out_send,
            recv_sem=out_recv.at[position // members], device_id=(ahead_of(position), leaf), device_id_type=MESH,
        ).start()
    received[0:2, :] = message[0:2, :]
    ctrl_all[leaf] = ctrl_ref[...]

    for fetch in fetches[6:]:
        fetch.wait()
    spare = jnp.zeros((HALF - 81, elements), F32)
    high, low = split(jnp.concatenate([vel_coef[...], spare], axis=0))
    coef[:HALF, :] = high
    coef[HALF:, :] = low

    low_half = lax.broadcasted_iota(jnp.int32, (8, LANES), 1) < LANES // 2
    low_rows = lax.broadcasted_iota(jnp.int32, (members, LANES), 1) < LANES // 2

    def share(buffer, send, recv, g):
        for i in range(1, peers):
            pltpu.make_async_remote_copy(
                src_ref=buffer.at[0, g], dst_ref=buffer.at[i, g], send_sem=send, recv_sem=recv.at[g],
                device_id=(me, leaf_peer(i)), device_id_type=MESH,
            ).start()

    def arrived(buffer, send, recv, g):
        pltpu.make_async_remote_copy(
            src_ref=buffer.at[1:, g], dst_ref=buffer.at[1:, g], send_sem=send, recv_sem=recv.at[g],
            device_id=(me, leaf_peer(1)), device_id_type=MESH,
        ).wait_recv()

    def tile(buffer, source, g, v):
        return buffer[source, g, v * ranks : (v + 1) * ranks, :]

    def gather(g, carry):
        def await_rows(count):
            pltpu.make_async_remote_copy(
                src_ref=message.at[:count, :], dst_ref=received.at[:count, :], send_sem=out_send,
                recv_sem=out_recv.at[g], device_id=(ahead_of(1), leaf), device_id_type=MESH,
            ).wait_recv()

        pl.when(g == 0)(lambda: await_rows(2 * members - 2))
        pl.when(g > 0)(lambda: await_rows(2 * members))
        rows = received[pl.ds(pl.multiple_of(2 * members * g, 2 * members), 2 * members), :]
        rows = jnp.transpose(jnp.concatenate([rows, rows], axis=0))
        values = [jnp.where(low_half, rows[16 * v : 16 * v + 8], rows[16 * v + 8 : 16 * v + 16]) for v in range(8)]
        for v in range(4):
            places[0, g, v * ranks : (v + 1) * ranks, :] = values[v]
        share(places, place_send, place_recv, g)

        for j in range(ranks // 2):
            pair = jnp.concatenate(
                [one_hot(values[0][r : r + 1], elements) for r in (2 * j, 2 * j + 1)], axis=1
            )
            taken = jnp.dot(coef[...], pair, preferred_element_type=F32)
            taken = taken[:HALF] + taken[HALF:]
            for i in range(2):
                at = (2 * j + i) * PITCH
                strided[at : at + HALF, :] = taken[:, i * LANES : (i + 1) * LANES]
        first, second, third = basis(values[1]), basis(values[2]), basis(values[3])
        plane = [x * y for x in second for y in third]
        for c in range(3):
            speed = None
            for a in range(3):
                inner = None
                for k in range(9):
                    term = plane[k] * strided[pl.ds(c * 27 + a * 9 + k, ranks, stride=PITCH), :]
                    inner = term if inner is None else inner + term
                inner = first[a] * inner
                speed = inner if speed is None else speed + inner
            forces[0, g, c * ranks : (c + 1) * ranks, :] = values[7] * (values[4 + c] - speed)
        share(forces, force_send, force_recv, g)

        for c in range(3):
            lower = tile(forces, 0, g, c)
            turned[c * 16 : c * 16 + 8, :] = lower
            turned[c * 16 + 8 : c * 16 + 16, :] = pltpu.roll(lower, LANES // 2, 1)
        flipped[...] = jnp.transpose(turned[...])[: 2 * members, :]
        even = flipped[pl.ds(0, members, stride=2), :]
        odd = flipped[pl.ds(1, members, stride=2), :]
        base = pl.multiple_of(g * members, members)
        answer[pl.ds(base, members), :] = jnp.where(low_rows, even, pltpu.roll(odd, LANES // 2, 1))
        for j in range(members - 1, -1, -1):
            steps = g * (members // 2) + (j + 1) // 2
            partner = lax.rem(me + (owners - steps if j % 2 else steps), owners)

            def reply(j=j, partner=partner):
                row = pl.ds(base + j, 1)
                pltpu.make_async_remote_copy(
                    src_ref=answer.at[row, :], dst_ref=returned.at[row, :], send_sem=back_sem.at[0],
                    recv_sem=back_sem.at[1], device_id=(partner, leaf), device_id_type=MESH,
                ).start()

            if j:
                reply()
            else:
                pl.when(g > 0)(reply)
        return carry

    corner = leaf.astype(F32) * float(per_leaf)

    def scatter(g):
        added = None
        for source in range(peers):
            first, second, third = (basis(tile(places, source, g, v)) for v in (1, 2, 3))
            plane = [x * y for x in second for y in third]
            half = source % 2 * (ranks * PITCH)
            for c in range(3):
                for a in range(3):
                    scaled = tile(forces, source, g, c) * first[a]
                    for k in range(9):
                        strided[pl.ds(half + c * 27 + a * 9 + k, ranks, stride=PITCH), :] = scaled * plane[k]
            near = tile(places, source, g, 0) - corner
            terms, hots = [], []
            for r in range(ranks):
                at = half + r * PITCH
                terms.append(jnp.concatenate(split(strided[at : at + HALF, :]), axis=0))
                hots.append(one_hot(near[r : r + 1], per_leaf))
            part = lax.dot_general(
                jnp.concatenate(hots, axis=1), jnp.concatenate(terms, axis=1), NT, preferred_element_type=F32
            )
            added = part if added is None else added + part
        total[:, : 2 * HALF] += added

    def contact():
        pltpu.make_async_remote_copy(
            src_ref=ctrl_all.at[: peers - 1], dst_ref=ctrl_all.at[: peers - 1], send_sem=ctrl_sem.at[0],
            recv_sem=ctrl_sem.at[1], device_id=(me, leaf_peer(1)), device_id_type=MESH,
        ).wait()
        zero7 = jnp.zeros((7, peers * patches), F32)
        whole = jnp.concatenate([ctrl_all[i] for i in range(peers)], axis=1)
        whole = jnp.concatenate([part for c in range(3) for part in (whole[c * 9 : (c + 1) * 9], zero7)], axis=0)
        ctrl_terms = jnp.concatenate(split(whole), axis=0)
        shell_k = lax.broadcasted_iota(jnp.int32, (16, 1), 0)
        contact_terms[...] = jnp.zeros_like(contact_terms)
        wide = 512

        def partners(start, size):
            return jnp.concatenate(
                [
                    one_hot(patch_ref[:, at : at + LANES].astype(F32), peers * patches)
                    for at in range(start, start + size, LANES)
                ],
                axis=1,
            )

        for j in range(points // wide):
            cols = slice(j * wide, (j + 1) * wide)
            taken = jnp.dot(ctrl_terms, partners(j * wide, wide), preferred_element_type=F32)
            taken = taken[:48] + taken[48:]
            weights = pick(shell_k // 3, basis(cparam_ref[0:1, cols])) * pick(
                lax.rem(shell_k, 3), basis(cparam_ref[1:2, cols])
            )
            weights = jnp.where(shell_k < 9, weights, 0.0)
            gap = [
                pos_ref[c : c + 1, cols] - jnp.sum(taken[c * 16 : (c + 1) * 16] * weights, axis=0, keepdims=True)
                for c in range(3)
            ]
            scale = STIFF / (1.0 + (gap[0] * gap[0] + gap[1] * gap[1] + gap[2] * gap[2]) / (REACH * REACH))
            for c in range(3):
                fc = scale * gap[c]
                push[c : c + 1, cols] = fc
                high, low = split(-(weights * fc))
                contact_terms[c * 16 : (c + 1) * 16, cols] = high
                contact_terms[64 + c * 16 : 64 + (c + 1) * 16, cols] = low
        reaction = lax.dot_general(partners(0, points), contact_terms[...], NT, preferred_element_type=F32)
        reaction = jnp.transpose(reaction)
        reaction = reaction[:48] + reaction[64:112]
        for q in range(peers):
            for c in range(3):
                patch_part[q, c * 9 : (c + 1) * 9, :] = reaction[c * 16 : c * 16 + 9, q * patches : (q + 1) * patches]
        for i in range(1, peers):
            pltpu.make_async_remote_copy(
                src_ref=patch_part.at[leaf_peer(i)], dst_ref=patch_all.at[leaf], send_sem=patch_sem.at[0],
                recv_sem=patch_sem.at[1], device_id=(me, leaf_peer(i)), device_id_type=MESH,
            ).start()
        patch_all[leaf] = patch_part[leaf]

    total[...] = jnp.zeros_like(total)
    turned[...] = jnp.zeros_like(turned)
    lax.fori_loop(0, GROUPS, gather, 0)
    returned[0:1, :] = answer[0:1, :]
    contact()
    strided[...] = jnp.zeros_like(strided)

    def gathered(g, carry):
        arrived(places, place_send, place_recv, g)
        arrived(forces, force_send, force_recv, g)
        scatter(g)
        return carry

    lax.fori_loop(0, GROUPS, gathered, 0)
    sums = jnp.transpose(total[...])
    flow_out[...] = sums[:81] + sums[HALF : HALF + 81]

    pltpu.make_async_remote_copy(
        src_ref=patch_part.at[: peers - 1], dst_ref=patch_all.at[: peers - 1], send_sem=patch_sem.at[0],
        recv_sem=patch_sem.at[1], device_id=(me, leaf_peer(1)), device_id_type=MESH,
    ).wait()
    patch_out[...] = (patch_all[0] + patch_all[1]) + (patch_all[2] + patch_all[3])

    pltpu.make_async_remote_copy(
        src_ref=answer.at[: owners - 1, :], dst_ref=returned.at[: owners - 1, :], send_sem=back_sem.at[0],
        recv_sem=back_sem.at[1], device_id=(ahead_of(1), leaf), device_id_type=MESH,
    ).wait()
    high, low = split(jnp.transpose(returned[...]))
    twice = jnp.concatenate([dest_hot[...], dest_hot[...]], axis=0)
    at_owner = jnp.dot(jnp.concatenate([high, low], axis=1), twice, preferred_element_type=F32)
    number = lax.broadcasted_iota(jnp.int32, (16, points), 0).astype(F32)
    for c in range(3):
        fsi = jnp.zeros((1, points), F32)
        for h in range(2):
            at = h * (LANES // 2) + c * 16
            mine = number == rank_row[...] - float(16 * h)
            fsi = fsi + jnp.sum(jnp.where(mine, at_owner[at : at + 16], 0.0), axis=0, keepdims=True)
        shell_out[c : c + 1, :] = push[c : c + 1, :] - fsi

    pltpu.make_async_remote_copy(
        src_ref=message.at[: 2 * (owners - 1), :], dst_ref=received.at[: 2 * (owners - 1), :], send_sem=out_send,
        recv_sem=out_recv.at[0], device_id=(ahead_of(1), leaf), device_id_type=MESH,
    ).wait_send()
    for buffer, send, recv in ((places, place_send, place_recv), (forces, force_send, force_recv)):
        pltpu.make_async_remote_copy(
            src_ref=buffer.at[1:], dst_ref=buffer.at[1:], send_sem=send, recv_sem=recv.at[0],
            device_id=(me, leaf_peer(1)), device_id_type=MESH,
        ).wait_send()


def finish(flow_in, shell_in, patch_in, flow_out, shell_out, patch_out):
    flow_out[...] = flow_in[...]
    shell_out[...] = shell_in[...]
    patch_out[...] = patch_in[...]


def solution(mesh):
    owners, peers = mesh.shape["flow"], mesh.shape["leaf"]

    def per_device(
        vel_coef, gp_block, gp_elem, gp_param, gp_vel, gp_weight, gp_pos, contact_patch, contact_param, patch_ctrl
    ):
        points, elements, patches = gp_elem.shape[0], vel_coef.shape[1], patch_ctrl.shape[1]
        per_leaf = elements // peers
        ranks = CAP * owners // GROUPS // LANES
        vmem = pl.BlockSpec(memory_space=pltpu.VMEM)
        outs = (
            jax.ShapeDtypeStruct((81, per_leaf), F32),
            jax.ShapeDtypeStruct((3, points), F32),
            jax.ShapeDtypeStruct((27, patches), F32),
        )
        arguments = (
            vel_coef,
            gp_block.reshape(1, points),
            gp_elem.reshape(1, points),
            gp_param,
            gp_vel,
            gp_weight.reshape(1, points),
            gp_pos,
            contact_patch.reshape(1, points),
            contact_param,
            patch_ctrl,
        )
        results = pl.pallas_call(
            kernel,
            out_shape=outs,
            in_specs=[pl.BlockSpec(memory_space=pl.ANY)] * 10,
            out_specs=(vmem,) * 3,
            scratch_shapes=[pltpu.VMEM(x.shape, x.dtype) for x in arguments]
            + [
                pltpu.VMEM((owners, points), BF16),
                pltpu.VMEM((1, points), F32),
                pltpu.VMEM((4 * LANES, points), BF16),
                pltpu.VMEM((2 * owners, LANES), F32),
                pltpu.VMEM((2 * owners, LANES), F32),
                pltpu.VMEM((peers, GROUPS, 4 * ranks, LANES), F32),
                pltpu.VMEM((2 * HALF, elements), BF16),
                pltpu.VMEM((peers, GROUPS, 3 * ranks, LANES), F32),
                pltpu.VMEM((LANES, LANES), F32),
                pltpu.VMEM((2 * owners // GROUPS, LANES), F32),
                pltpu.VMEM((owners, LANES), F32),
                pltpu.VMEM((owners, LANES), F32),
                pltpu.VMEM((2 * ranks * PITCH, LANES), F32),
                pltpu.VMEM((per_leaf, 2 * LANES), F32),
                pltpu.VMEM((LANES, points), BF16),
                pltpu.VMEM((3, points), F32),
                pltpu.VMEM((peers, 27, patches), F32),
                pltpu.VMEM((peers, 27, patches), F32),
                pltpu.VMEM((peers, 27, patches), F32),
                pltpu.SemaphoreType.DMA((10,)),
                pltpu.SemaphoreType.DMA,
                pltpu.SemaphoreType.DMA((GROUPS,)),
                pltpu.SemaphoreType.DMA((2,)),
                pltpu.SemaphoreType.DMA((2,)),
                pltpu.SemaphoreType.DMA((2,)),
                pltpu.SemaphoreType.DMA,
                pltpu.SemaphoreType.DMA((GROUPS,)),
                pltpu.SemaphoreType.DMA,
                pltpu.SemaphoreType.DMA((GROUPS,)),
            ],
            compiler_params=pltpu.CompilerParams(
                collective_id=0, has_side_effects=True, vmem_limit_bytes=60 * 1024 * 1024
            ),
        )(*arguments)
        return pl.pallas_call(finish, out_shape=outs, in_specs=[vmem] * 3, out_specs=(vmem,) * 3)(*results)

    both = ("flow", "leaf")
    return jax.shard_map(
        per_device,
        mesh=mesh,
        in_specs=(
            P(None, "flow"), P(both, None), P(both), P(None, both), P(None, both),
            P(both), P(None, both), P(both), P(None, both), P(None, both),
        ),
        out_specs=(P(None, both), P(None, both), P(None, both)),
        check_vma=False,
    )
```

```python
import jax
import jax.numpy as jnp
from jax import lax
from jax.experimental import pallas as pl
from jax.experimental.pallas import tpu as pltpu
from jax.sharding import PartitionSpec as P

BETA = 1.5
STIFF = 2.0
REACH = 0.5
CAP = 32
LANES = 128
GROUPS = 4
HALF = 96
PITCH = 104
F32 = jnp.float32
BF16 = jnp.bfloat16
MESH = pl.DeviceIdType.MESH
NT = (((1,), (1,)), ((), ()))


def split(x):
    high = x.astype(BF16)
    return high, (x - high.astype(F32)).astype(BF16)


def basis(x):
    return (0.5 * (1.0 - x) ** 2, 0.5 * (1.0 + 2.0 * x - 2.0 * x * x), 0.5 * x * x)


def pick(digit, values):
    return jnp.where(digit == 0, values[0], jnp.where(digit == 1, values[1], values[2]))


def one_hot(row, rows):
    step = min(rows, 256)
    number = lax.broadcasted_iota(jnp.int32, (step, LANES), 0).astype(F32).astype(BF16)
    one, zero = jnp.ones((step, LANES), BF16), jnp.zeros((step, LANES), BF16)
    out = []
    for first in range(0, rows, step):
        near = jnp.broadcast_to(row - float(first), (16, LANES)).astype(BF16)
        near = jnp.concatenate([near] * (step // 16), axis=0)
        out.append(jnp.where(number == near, one, zero))
    return jnp.concatenate(out, axis=0) if len(out) > 1 else out[0]


def kernel(
    vel_coef_hbm, dest_hbm, elem_hbm, param_hbm, vel_hbm, weight_hbm, pos_hbm, patch_hbm, cparam_hbm, ctrl_hbm,
    flow_out, shell_out, patch_out,
    vel_coef, dest_ref, elem_ref, param_ref, vel_ref, weight_ref, pos_ref, patch_ref, cparam_ref, ctrl_ref,
    dest_hot, rank_row, packed, message, received, places, coef, forces, turned, flipped, answer, returned,
    strided, total, contact_terms, push, ctrl_all, patch_part, patch_all,
    in_sem, out_send, out_recv, back_sem, ctrl_sem, patch_sem, place_send, place_recv, force_send, force_recv,
):
    owners, peers = lax.axis_size("flow"), lax.axis_size("leaf")
    me, leaf = lax.axis_index("flow"), lax.axis_index("leaf")
    points = dest_ref.shape[1]
    elements = vel_coef.shape[1]
    per_leaf = elements // peers
    patches = ctrl_ref.shape[1]
    members = owners // GROUPS
    ranks = CAP * members // LANES

    def offset(position):
        return (position + 1) // 2 if position % 2 else (owners - position // 2) % owners

    def ahead_of(position):
        return lax.rem(me + offset(position), owners)

    def behind(position):
        return lax.rem(me + (owners - offset(position)), owners)

    def leaf_peer(i):
        return lax.rem(leaf + i, peers)

    inputs = [
        (dest_hbm, dest_ref), (elem_hbm, elem_ref), (param_hbm, param_ref), (vel_hbm, vel_ref),
        (weight_hbm, weight_ref), (ctrl_hbm, ctrl_ref), (patch_hbm, patch_ref), (pos_hbm, pos_ref),
        (cparam_hbm, cparam_ref), (vel_coef_hbm, vel_coef),
    ]
    fetches = [pltpu.make_async_copy(src, dst, in_sem.at[i]) for i, (src, dst) in enumerate(inputs)]
    for fetch in fetches:
        fetch.start()
    barrier = pltpu.get_barrier_semaphore()
    for position in range(owners - 1, 0, -1):
        pl.semaphore_signal(barrier, inc=1, device_id=(behind(position), leaf), device_id_type=MESH)
    for i in range(1, peers):
        pl.semaphore_signal(barrier, inc=1, device_id=(me, leaf_peer(i)), device_id_type=MESH)

    for fetch in fetches[:6]:
        fetch.wait()
    position = lax.broadcasted_iota(jnp.int32, (owners, 1), 0)
    distance = jnp.where(
        lax.rem(position, 2) == 1, (position + 1) // 2, jnp.where(position == 0, 0, owners - position // 2)
    )
    away = dest_ref[...] - me
    away = jnp.where(away < 0, away + owners, away)
    dest_hot[...] = jnp.where(distance == away, 1.0, 0.0).astype(BF16)
    block = 256
    before = (
        lax.broadcasted_iota(jnp.int32, (block, block), 0) < lax.broadcasted_iota(jnp.int32, (block, block), 1)
    ).astype(F32).astype(BF16)
    carry = jnp.zeros((owners, 1), F32)
    for b in range(points // block):
        part = dest_hot[:, b * block : (b + 1) * block]
        earlier = jnp.dot(part, before, preferred_element_type=F32)
        wide = part.astype(F32)
        rank_row[:, b * block : (b + 1) * block] = jnp.sum(wide * (earlier + carry), axis=0, keepdims=True)
        carry = carry + jnp.sum(wide, axis=1, keepdims=True)

    rank_hot = lax.broadcasted_iota(jnp.int32, (CAP, points), 0).astype(F32) == rank_row[...]
    values = [elem_ref[...].astype(F32)]
    values += [param_ref[i : i + 1, :] for i in range(3)]
    values += [vel_ref[i : i + 1, :] for i in range(3)]
    values += [BETA * weight_ref[...]]
    for v, value in enumerate(values):
        high = value.astype(BF16).astype(F32)
        for h in range(2):
            chosen = rank_hot[h * 16 : (h + 1) * 16]
            at = h * LANES + v * 16
            packed[at : at + 16, :] = jnp.where(chosen, high, 0.0).astype(BF16)
            packed[2 * LANES + at : 2 * LANES + at + 16, :] = jnp.where(chosen, value - high, 0.0).astype(BF16)
    spread = lax.dot_general(packed[...], dest_hot[...], NT, preferred_element_type=F32)
    spread = spread[: 2 * LANES] + spread[2 * LANES :]
    for h in range(2):
        message[pl.ds(h, owners, stride=2), :] = jnp.transpose(spread[h * LANES : (h + 1) * LANES])

    pl.semaphore_wait(barrier, owners - 1 + peers - 1)

    ctrl_copies = [
        pltpu.make_async_remote_copy(
            src_ref=ctrl_ref, dst_ref=ctrl_all.at[leaf], send_sem=ctrl_sem.at[0], recv_sem=ctrl_sem.at[1],
            device_id=(me, leaf_peer(i)), device_id_type=MESH,
        )
        for i in range(1, peers)
    ]
    for copy in ctrl_copies:
        copy.start()
    for position in [g * members + j for g in (3, 0, 2, 1) for j in range(members - 1, -1, -1) if g or j]:
        rows = pl.ds(2 * position, 2)
        pltpu.make_async_remote_copy(
            src_ref=message.at[rows, :], dst_ref=received.at[rows, :], send_sem=out_send,
            recv_sem=out_recv.at[position // members], device_id=(ahead_of(position), leaf), device_id_type=MESH,
        ).start()
    received[0:2, :] = message[0:2, :]
    ctrl_all[leaf] = ctrl_ref[...]

    for fetch in fetches[6:]:
        fetch.wait()
    spare = jnp.zeros((HALF - 81, elements), F32)
    high, low = split(jnp.concatenate([vel_coef[...], spare], axis=0))
    coef[:HALF, :] = high
    coef[HALF:, :] = low

    low_half = lax.broadcasted_iota(jnp.int32, (8, LANES), 1) < LANES // 2
    low_rows = lax.broadcasted_iota(jnp.int32, (members, LANES), 1) < LANES // 2

    def share(buffer, send, recv, g):
        for i in range(1, peers):
            pltpu.make_async_remote_copy(
                src_ref=buffer.at[0, g], dst_ref=buffer.at[i, g], send_sem=send, recv_sem=recv.at[g],
                device_id=(me, leaf_peer(i)), device_id_type=MESH,
            ).start()

    def arrived(buffer, send, recv, g):
        pltpu.make_async_remote_copy(
            src_ref=buffer.at[1:, g], dst_ref=buffer.at[1:, g], send_sem=send, recv_sem=recv.at[g],
            device_id=(me, leaf_peer(1)), device_id_type=MESH,
        ).wait_recv()

    def tile(buffer, source, g, v):
        return buffer[source, g, v * ranks : (v + 1) * ranks, :]

    def turn(i):
        return lax.rem(GROUPS - i, GROUPS)

    def gather(i, carry):
        g = turn(i)

        def await_rows(count):
            pltpu.make_async_remote_copy(
                src_ref=message.at[:count, :], dst_ref=received.at[:count, :], send_sem=out_send,
                recv_sem=out_recv.at[g], device_id=(ahead_of(1), leaf), device_id_type=MESH,
            ).wait_recv()

        pl.when(g == 0)(lambda: await_rows(2 * members - 2))
        pl.when(g > 0)(lambda: await_rows(2 * members))
        rows = received[pl.ds(pl.multiple_of(2 * members * g, 2 * members), 2 * members), :]
        rows = jnp.transpose(jnp.concatenate([rows, rows], axis=0))
        values = [jnp.where(low_half, rows[16 * v : 16 * v + 8], rows[16 * v + 8 : 16 * v + 16]) for v in range(8)]
        for v in range(4):
            places[0, g, v * ranks : (v + 1) * ranks, :] = values[v]
        share(places, place_send, place_recv, g)

        for j in range(ranks // 2):
            pair = jnp.concatenate(
                [one_hot(values[0][r : r + 1], elements) for r in (2 * j, 2 * j + 1)], axis=1
            )
            taken = jnp.dot(coef[...], pair, preferred_element_type=F32)
            taken = taken[:HALF] + taken[HALF:]
            for i in range(2):
                at = (2 * j + i) * PITCH
                strided[at : at + HALF, :] = taken[:, i * LANES : (i + 1) * LANES]
        first, second, third = basis(values[1]), basis(values[2]), basis(values[3])
        plane = [x * y for x in second for y in third]
        for c in range(3):
            speed = None
            for a in range(3):
                inner = None
                for k in range(9):
                    term = plane[k] * strided[pl.ds(c * 27 + a * 9 + k, ranks, stride=PITCH), :]
                    inner = term if inner is None else inner + term
                inner = first[a] * inner
                speed = inner if speed is None else speed + inner
            forces[0, g, c * ranks : (c + 1) * ranks, :] = values[7] * (values[4 + c] - speed)
        share(forces, force_send, force_recv, g)

        for c in range(3):
            lower = tile(forces, 0, g, c)
            turned[c * 16 : c * 16 + 8, :] = lower
            turned[c * 16 + 8 : c * 16 + 16, :] = pltpu.roll(lower, LANES // 2, 1)
        flipped[...] = jnp.transpose(turned[...])[: 2 * members, :]
        even = flipped[pl.ds(0, members, stride=2), :]
        odd = flipped[pl.ds(1, members, stride=2), :]
        base = pl.multiple_of(g * members, members)
        answer[pl.ds(base, members), :] = jnp.where(low_rows, even, pltpu.roll(odd, LANES // 2, 1))
        for j in range(members - 1, -1, -1):
            steps = g * (members // 2) + (j + 1) // 2
            partner = lax.rem(me + (owners - steps if j % 2 else steps), owners)

            def reply(j=j, partner=partner):
                row = pl.ds(base + j, 1)
                pltpu.make_async_remote_copy(
                    src_ref=answer.at[row, :], dst_ref=returned.at[row, :], send_sem=back_sem.at[0],
                    recv_sem=back_sem.at[1], device_id=(partner, leaf), device_id_type=MESH,
                ).start()

            if j:
                reply()
            else:
                pl.when(g > 0)(reply)
        return carry

    corner = leaf.astype(F32) * float(per_leaf)

    def scatter(g):
        added = None
        for source in range(peers):
            first, second, third = (basis(tile(places, source, g, v)) for v in (1, 2, 3))
            plane = [x * y for x in second for y in third]
            half = source % 2 * (ranks * PITCH)
            for c in range(3):
                for a in range(3):
                    scaled = tile(forces, source, g, c) * first[a]
                    for k in range(9):
                        strided[pl.ds(half + c * 27 + a * 9 + k, ranks, stride=PITCH), :] = scaled * plane[k]
            near = tile(places, source, g, 0) - corner
            terms, hots = [], []
            for r in range(ranks):
                at = half + r * PITCH
                terms.append(jnp.concatenate(split(strided[at : at + HALF, :]), axis=0))
                hots.append(one_hot(near[r : r + 1], per_leaf))
            part = lax.dot_general(
                jnp.concatenate(hots, axis=1), jnp.concatenate(terms, axis=1), NT, preferred_element_type=F32
            )
            added = part if added is None else added + part
        total[:, : 2 * HALF] += added

    def contact():
        pltpu.make_async_remote_copy(
            src_ref=ctrl_all.at[: peers - 1], dst_ref=ctrl_all.at[: peers - 1], send_sem=ctrl_sem.at[0],
            recv_sem=ctrl_sem.at[1], device_id=(me, leaf_peer(1)), device_id_type=MESH,
        ).wait()
        zero7 = jnp.zeros((7, peers * patches), F32)
        whole = jnp.concatenate([ctrl_all[i] for i in range(peers)], axis=1)
        whole = jnp.concatenate([part for c in range(3) for part in (whole[c * 9 : (c + 1) * 9], zero7)], axis=0)
        ctrl_terms = jnp.concatenate(split(whole), axis=0)
        shell_k = lax.broadcasted_iota(jnp.int32, (16, 1), 0)
        contact_terms[...] = jnp.zeros_like(contact_terms)
        wide = 512

        def partners(start, size):
            return jnp.concatenate(
                [
                    one_hot(patch_ref[:, at : at + LANES].astype(F32), peers * patches)
                    for at in range(start, start + size, LANES)
                ],
                axis=1,
            )

        for j in range(points // wide):
            cols = slice(j * wide, (j + 1) * wide)
            taken = jnp.dot(ctrl_terms, partners(j * wide, wide), preferred_element_type=F32)
            taken = taken[:48] + taken[48:]
            weights = pick(shell_k // 3, basis(cparam_ref[0:1, cols])) * pick(
                lax.rem(shell_k, 3), basis(cparam_ref[1:2, cols])
            )
            weights = jnp.where(shell_k < 9, weights, 0.0)
            gap = [
                pos_ref[c : c + 1, cols] - jnp.sum(taken[c * 16 : (c + 1) * 16] * weights, axis=0, keepdims=True)
                for c in range(3)
            ]
            scale = STIFF / (1.0 + (gap[0] * gap[0] + gap[1] * gap[1] + gap[2] * gap[2]) / (REACH * REACH))
            for c in range(3):
                fc = scale * gap[c]
                push[c : c + 1, cols] = fc
                high, low = split(-(weights * fc))
                contact_terms[c * 16 : (c + 1) * 16, cols] = high
                contact_terms[64 + c * 16 : 64 + (c + 1) * 16, cols] = low
        reaction = lax.dot_general(partners(0, points), contact_terms[...], NT, preferred_element_type=F32)
        reaction = jnp.transpose(reaction)
        reaction = reaction[:48] + reaction[64:112]
        for q in range(peers):
            for c in range(3):
                patch_part[q, c * 9 : (c + 1) * 9, :] = reaction[c * 16 : c * 16 + 9, q * patches : (q + 1) * patches]
        for i in range(1, peers):
            pltpu.make_async_remote_copy(
                src_ref=patch_part.at[leaf_peer(i)], dst_ref=patch_all.at[leaf], send_sem=patch_sem.at[0],
                recv_sem=patch_sem.at[1], device_id=(me, leaf_peer(i)), device_id_type=MESH,
            ).start()
        patch_all[leaf] = patch_part[leaf]

    total[...] = jnp.zeros_like(total)
    turned[...] = jnp.zeros_like(turned)
    contact()
    lax.fori_loop(0, GROUPS, gather, 0)
    returned[0:1, :] = answer[0:1, :]
    strided[...] = jnp.zeros_like(strided)

    def gathered(i, carry):
        g = turn(i)
        arrived(places, place_send, place_recv, g)
        arrived(forces, force_send, force_recv, g)
        scatter(g)
        return carry

    lax.fori_loop(0, GROUPS, gathered, 0)
    sums = jnp.transpose(total[...])
    flow_out[...] = sums[:81] + sums[HALF : HALF + 81]

    pltpu.make_async_remote_copy(
        src_ref=patch_part.at[: peers - 1], dst_ref=patch_all.at[: peers - 1], send_sem=patch_sem.at[0],
        recv_sem=patch_sem.at[1], device_id=(me, leaf_peer(1)), device_id_type=MESH,
    ).wait()
    patch_out[...] = (patch_all[0] + patch_all[1]) + (patch_all[2] + patch_all[3])

    pltpu.make_async_remote_copy(
        src_ref=answer.at[: owners - 1, :], dst_ref=returned.at[: owners - 1, :], send_sem=back_sem.at[0],
        recv_sem=back_sem.at[1], device_id=(ahead_of(1), leaf), device_id_type=MESH,
    ).wait()
    high, low = split(jnp.transpose(returned[...]))
    twice = jnp.concatenate([dest_hot[...], dest_hot[...]], axis=0)
    at_owner = jnp.dot(jnp.concatenate([high, low], axis=1), twice, preferred_element_type=F32)
    number = lax.broadcasted_iota(jnp.int32, (16, points), 0).astype(F32)
    for c in range(3):
        fsi = jnp.zeros((1, points), F32)
        for h in range(2):
            at = h * (LANES // 2) + c * 16
            mine = number == rank_row[...] - float(16 * h)
            fsi = fsi + jnp.sum(jnp.where(mine, at_owner[at : at + 16], 0.0), axis=0, keepdims=True)
        shell_out[c : c + 1, :] = push[c : c + 1, :] - fsi

    pltpu.make_async_remote_copy(
        src_ref=message.at[: 2 * (owners - 1), :], dst_ref=received.at[: 2 * (owners - 1), :], send_sem=out_send,
        recv_sem=out_recv.at[0], device_id=(ahead_of(1), leaf), device_id_type=MESH,
    ).wait_send()
    for buffer, send, recv in ((places, place_send, place_recv), (forces, force_send, force_recv)):
        pltpu.make_async_remote_copy(
            src_ref=buffer.at[1:], dst_ref=buffer.at[1:], send_sem=send, recv_sem=recv.at[0],
            device_id=(me, leaf_peer(1)), device_id_type=MESH,
        ).wait_send()


def finish(flow_in, shell_in, patch_in, flow_out, shell_out, patch_out, sems):
    copies = [
        pltpu.make_async_copy(src, dst, sems.at[i])
        for i, (src, dst) in enumerate(((flow_in, flow_out), (shell_in, shell_out), (patch_in, patch_out)))
    ]
    for copy in copies:
        copy.start()
    for copy in copies:
        copy.wait()


def solution(mesh):
    owners, peers = mesh.shape["flow"], mesh.shape["leaf"]

    def per_device(
        vel_coef, gp_block, gp_elem, gp_param, gp_vel, gp_weight, gp_pos, contact_patch, contact_param, patch_ctrl
    ):
        points, elements, patches = gp_elem.shape[0], vel_coef.shape[1], patch_ctrl.shape[1]
        per_leaf = elements // peers
        ranks = CAP * owners // GROUPS // LANES
        vmem = pl.BlockSpec(memory_space=pltpu.VMEM)
        outs = (
            jax.ShapeDtypeStruct((81, per_leaf), F32),
            jax.ShapeDtypeStruct((3, points), F32),
            jax.ShapeDtypeStruct((27, patches), F32),
        )
        arguments = (
            vel_coef,
            gp_block.reshape(1, points),
            gp_elem.reshape(1, points),
            gp_param,
            gp_vel,
            gp_weight.reshape(1, points),
            gp_pos,
            contact_patch.reshape(1, points),
            contact_param,
            patch_ctrl,
        )
        results = pl.pallas_call(
            kernel,
            out_shape=tuple(pltpu.VMEM(x.shape, x.dtype) for x in outs),
            in_specs=[pl.BlockSpec(memory_space=pl.ANY)] * 10,
            out_specs=(vmem,) * 3,
            scratch_shapes=[pltpu.VMEM(x.shape, x.dtype) for x in arguments]
            + [
                pltpu.VMEM((owners, points), BF16),
                pltpu.VMEM((1, points), F32),
                pltpu.VMEM((4 * LANES, points), BF16),
                pltpu.VMEM((2 * owners, LANES), F32),
                pltpu.VMEM((2 * owners, LANES), F32),
                pltpu.VMEM((peers, GROUPS, 4 * ranks, LANES), F32),
                pltpu.VMEM((2 * HALF, elements), BF16),
                pltpu.VMEM((peers, GROUPS, 3 * ranks, LANES), F32),
                pltpu.VMEM((LANES, LANES), F32),
                pltpu.VMEM((2 * owners // GROUPS, LANES), F32),
                pltpu.VMEM((owners, LANES), F32),
                pltpu.VMEM((owners, LANES), F32),
                pltpu.VMEM((2 * ranks * PITCH, LANES), F32),
                pltpu.VMEM((per_leaf, 2 * LANES), F32),
                pltpu.VMEM((LANES, points), BF16),
                pltpu.VMEM((3, points), F32),
                pltpu.VMEM((peers, 27, patches), F32),
                pltpu.VMEM((peers, 27, patches), F32),
                pltpu.VMEM((peers, 27, patches), F32),
                pltpu.SemaphoreType.DMA((10,)),
                pltpu.SemaphoreType.DMA,
                pltpu.SemaphoreType.DMA((GROUPS,)),
                pltpu.SemaphoreType.DMA((2,)),
                pltpu.SemaphoreType.DMA((2,)),
                pltpu.SemaphoreType.DMA((2,)),
                pltpu.SemaphoreType.DMA,
                pltpu.SemaphoreType.DMA((GROUPS,)),
                pltpu.SemaphoreType.DMA,
                pltpu.SemaphoreType.DMA((GROUPS,)),
            ],
            compiler_params=pltpu.CompilerParams(
                collective_id=0, has_side_effects=True, vmem_limit_bytes=60 * 1024 * 1024
            ),
        )(*arguments)
        return pl.pallas_call(
            finish,
            out_shape=outs,
            in_specs=[vmem] * 3,
            out_specs=(pl.BlockSpec(memory_space=pl.ANY),) * 3,
            scratch_shapes=[pltpu.SemaphoreType.DMA((3,))],
        )(
            *[pltpu.with_memory_space_constraint(x, pltpu.VMEM) for x in results]
        )

    both = ("flow", "leaf")
    return jax.shard_map(
        per_device,
        mesh=mesh,
        in_specs=(
            P(None, "flow"), P(both, None), P(both), P(None, both), P(None, both),
            P(both), P(None, both), P(both), P(None, both), P(None, both),
        ),
        out_specs=(P(None, both), P(None, both), P(None, both)),
        check_vma=False,
    )
```

```python
import jax
import jax.numpy as jnp
from jax import lax
from jax.experimental import pallas as pl
from jax.experimental.pallas import tpu as pltpu
from jax.sharding import PartitionSpec as P

BETA = 1.5
STIFF = 2.0
REACH = 0.5
CAP = 32
LANES = 128
GROUPS = 4
HALF = 96
PITCH = 104
F32 = jnp.float32
BF16 = jnp.bfloat16
MESH = pl.DeviceIdType.MESH
NT = (((1,), (1,)), ((), ()))


def split(x):
    high = x.astype(BF16)
    return high, (x - high.astype(F32)).astype(BF16)


def basis(x):
    return (0.5 * (1.0 - x) ** 2, 0.5 * (1.0 + 2.0 * x - 2.0 * x * x), 0.5 * x * x)


def pick(digit, values):
    return jnp.where(digit == 0, values[0], jnp.where(digit == 1, values[1], values[2]))


def one_hot(row, rows):
    step = min(rows, 256)
    number = lax.broadcasted_iota(jnp.int32, (step, LANES), 0).astype(F32).astype(BF16)
    one, zero = jnp.ones((step, LANES), BF16), jnp.zeros((step, LANES), BF16)
    out = []
    for first in range(0, rows, step):
        near = jnp.broadcast_to(row - float(first), (16, LANES)).astype(BF16)
        near = jnp.concatenate([near] * (step // 16), axis=0)
        out.append(jnp.where(number == near, one, zero))
    return jnp.concatenate(out, axis=0) if len(out) > 1 else out[0]


def kernel(
    vel_coef_hbm, dest_hbm, elem_hbm, param_hbm, vel_hbm, weight_hbm, pos_hbm, patch_hbm, cparam_hbm, ctrl_hbm,
    flow_out, shell_out, patch_out,
    vel_coef, dest_ref, elem_ref, param_ref, vel_ref, weight_ref, pos_ref, patch_ref, cparam_ref, ctrl_ref,
    dest_hot, rank_row, packed, message, received, places, coef, forces, turned, flipped, answer, returned,
    strided, total, contact_terms, push, ctrl_all, patch_part, patch_all,
    in_sem, out_send, out_recv, back_sem, ctrl_sem, patch_sem, place_send, place_recv, force_send, force_recv,
):
    owners, peers = lax.axis_size("flow"), lax.axis_size("leaf")
    me, leaf = lax.axis_index("flow"), lax.axis_index("leaf")
    points = dest_ref.shape[1]
    elements = vel_coef.shape[1]
    per_leaf = elements // peers
    patches = ctrl_ref.shape[1]
    members = owners // GROUPS
    ranks = CAP * members // LANES

    def offset(position):
        return (position + 1) // 2 if position % 2 else (owners - position // 2) % owners

    def ahead_of(position):
        return lax.rem(me + offset(position), owners)

    def behind(position):
        return lax.rem(me + (owners - offset(position)), owners)

    def leaf_peer(i):
        return lax.rem(leaf + i, peers)

    inputs = [
        (dest_hbm, dest_ref), (elem_hbm, elem_ref), (param_hbm, param_ref), (vel_hbm, vel_ref),
        (weight_hbm, weight_ref), (ctrl_hbm, ctrl_ref), (patch_hbm, patch_ref), (pos_hbm, pos_ref),
        (cparam_hbm, cparam_ref), (vel_coef_hbm, vel_coef),
    ]
    fetches = [pltpu.make_async_copy(src, dst, in_sem.at[i]) for i, (src, dst) in enumerate(inputs)]
    for fetch in fetches:
        fetch.start()
    barrier = pltpu.get_barrier_semaphore()
    for position in range(owners - 1, 0, -1):
        pl.semaphore_signal(barrier, inc=1, device_id=(behind(position), leaf), device_id_type=MESH)
    for i in range(1, peers):
        pl.semaphore_signal(barrier, inc=1, device_id=(me, leaf_peer(i)), device_id_type=MESH)

    for fetch in fetches[:6]:
        fetch.wait()
    position = lax.broadcasted_iota(jnp.int32, (owners, 1), 0)
    distance = jnp.where(
        lax.rem(position, 2) == 1, (position + 1) // 2, jnp.where(position == 0, 0, owners - position // 2)
    )
    away = dest_ref[...] - me
    away = jnp.where(away < 0, away + owners, away)
    dest_hot[...] = jnp.where(distance == away, 1.0, 0.0).astype(BF16)
    block = 256
    before = (
        lax.broadcasted_iota(jnp.int32, (block, block), 0) < lax.broadcasted_iota(jnp.int32, (block, block), 1)
    ).astype(F32).astype(BF16)
    carry = jnp.zeros((owners, 1), F32)
    for b in range(points // block):
        part = dest_hot[:, b * block : (b + 1) * block]
        earlier = jnp.dot(part, before, preferred_element_type=F32)
        wide = part.astype(F32)
        rank_row[:, b * block : (b + 1) * block] = jnp.sum(wide * (earlier + carry), axis=0, keepdims=True)
        carry = carry + jnp.sum(wide, axis=1, keepdims=True)

    rank_hot = lax.broadcasted_iota(jnp.int32, (CAP, points), 0).astype(F32) == rank_row[...]
    values = [elem_ref[...].astype(F32)]
    values += [param_ref[i : i + 1, :] for i in range(3)]
    values += [vel_ref[i : i + 1, :] for i in range(3)]
    values += [BETA * weight_ref[...]]
    for v, value in enumerate(values):
        high = value.astype(BF16).astype(F32)
        for h in range(2):
            chosen = rank_hot[h * 16 : (h + 1) * 16]
            at = h * LANES + v * 16
            packed[at : at + 16, :] = jnp.where(chosen, high, 0.0).astype(BF16)
            packed[2 * LANES + at : 2 * LANES + at + 16, :] = jnp.where(chosen, value - high, 0.0).astype(BF16)
    spread = lax.dot_general(packed[...], dest_hot[...], NT, preferred_element_type=F32)
    spread = spread[: 2 * LANES] + spread[2 * LANES :]
    for h in range(2):
        message[pl.ds(h, owners, stride=2), :] = jnp.transpose(spread[h * LANES : (h + 1) * LANES])

    pl.semaphore_wait(barrier, owners - 1 + peers - 1)

    ctrl_copies = [
        pltpu.make_async_remote_copy(
            src_ref=ctrl_ref, dst_ref=ctrl_all.at[leaf], send_sem=ctrl_sem.at[0], recv_sem=ctrl_sem.at[1],
            device_id=(me, leaf_peer(i)), device_id_type=MESH,
        )
        for i in range(1, peers)
    ]
    for copy in ctrl_copies:
        copy.start()
    for position in [g * members + j for g in (0, 3, 2, 1) for j in range(members - 1, -1, -1) if g or j]:
        rows = pl.ds(2 * position, 2)
        pltpu.make_async_remote_copy(
            src_ref=message.at[rows, :], dst_ref=received.at[rows, :], send_sem=out_send,
            recv_sem=out_recv.at[position // members], device_id=(ahead_of(position), leaf), device_id_type=MESH,
        ).start()
    received[0:2, :] = message[0:2, :]
    ctrl_all[leaf] = ctrl_ref[...]

    for fetch in fetches[6:]:
        fetch.wait()
    spare = jnp.zeros((HALF - 81, elements), F32)
    high, low = split(jnp.concatenate([vel_coef[...], spare], axis=0))
    coef[:HALF, :] = high
    coef[HALF:, :] = low

    low_half = lax.broadcasted_iota(jnp.int32, (8, LANES), 1) < LANES // 2
    low_rows = lax.broadcasted_iota(jnp.int32, (members, LANES), 1) < LANES // 2

    def share(buffer, send, recv, g):
        for i in range(1, peers):
            pltpu.make_async_remote_copy(
                src_ref=buffer.at[0, g], dst_ref=buffer.at[i, g], send_sem=send, recv_sem=recv.at[g],
                device_id=(me, leaf_peer(i)), device_id_type=MESH,
            ).start()

    def arrived(buffer, send, recv, g):
        pltpu.make_async_remote_copy(
            src_ref=buffer.at[1:, g], dst_ref=buffer.at[1:, g], send_sem=send, recv_sem=recv.at[g],
            device_id=(me, leaf_peer(1)), device_id_type=MESH,
        ).wait_recv()

    def tile(buffer, source, g, v):
        return buffer[source, g, v * ranks : (v + 1) * ranks, :]

    def turn(i):
        return lax.rem(GROUPS - i, GROUPS)

    def contact():
        pltpu.make_async_remote_copy(
            src_ref=ctrl_all.at[: peers - 1], dst_ref=ctrl_all.at[: peers - 1], send_sem=ctrl_sem.at[0],
            recv_sem=ctrl_sem.at[1], device_id=(me, leaf_peer(1)), device_id_type=MESH,
        ).wait()
        zero7 = jnp.zeros((7, peers * patches), F32)
        whole = jnp.concatenate([ctrl_all[i] for i in range(peers)], axis=1)
        whole = jnp.concatenate([part for c in range(3) for part in (whole[c * 9 : (c + 1) * 9], zero7)], axis=0)
        ctrl_terms = jnp.concatenate(split(whole), axis=0)
        shell_k = lax.broadcasted_iota(jnp.int32, (16, 1), 0)
        contact_terms[...] = jnp.zeros_like(contact_terms)
        wide = 512

        def partners(start, size):
            return jnp.concatenate(
                [
                    one_hot(patch_ref[:, at : at + LANES].astype(F32), peers * patches)
                    for at in range(start, start + size, LANES)
                ],
                axis=1,
            )

        for j in range(points // wide):
            cols = slice(j * wide, (j + 1) * wide)
            taken = jnp.dot(ctrl_terms, partners(j * wide, wide), preferred_element_type=F32)
            taken = taken[:48] + taken[48:]
            weights = pick(shell_k // 3, basis(cparam_ref[0:1, cols])) * pick(
                lax.rem(shell_k, 3), basis(cparam_ref[1:2, cols])
            )
            weights = jnp.where(shell_k < 9, weights, 0.0)
            gap = [
                pos_ref[c : c + 1, cols] - jnp.sum(taken[c * 16 : (c + 1) * 16] * weights, axis=0, keepdims=True)
                for c in range(3)
            ]
            scale = STIFF / (1.0 + (gap[0] * gap[0] + gap[1] * gap[1] + gap[2] * gap[2]) / (REACH * REACH))
            for c in range(3):
                fc = scale * gap[c]
                push[c : c + 1, cols] = fc
                high, low = split(-(weights * fc))
                contact_terms[c * 16 : (c + 1) * 16, cols] = high
                contact_terms[64 + c * 16 : 64 + (c + 1) * 16, cols] = low
        reaction = lax.dot_general(partners(0, points), contact_terms[...], NT, preferred_element_type=F32)
        reaction = jnp.transpose(reaction)
        reaction = reaction[:48] + reaction[64:112]
        for q in range(peers):
            for c in range(3):
                patch_part[q, c * 9 : (c + 1) * 9, :] = reaction[c * 16 : c * 16 + 9, q * patches : (q + 1) * patches]
        for i in range(1, peers):
            pltpu.make_async_remote_copy(
                src_ref=patch_part.at[leaf_peer(i)], dst_ref=patch_all.at[leaf], send_sem=patch_sem.at[0],
                recv_sem=patch_sem.at[1], device_id=(me, leaf_peer(i)), device_id_type=MESH,
            ).start()
        patch_all[leaf] = patch_part[leaf]

    def gather(order, carry):
        g = turn(order)

        def await_rows(count):
            pltpu.make_async_remote_copy(
                src_ref=message.at[:count, :], dst_ref=received.at[:count, :], send_sem=out_send,
                recv_sem=out_recv.at[g], device_id=(ahead_of(1), leaf), device_id_type=MESH,
            ).wait_recv()

        pl.when(g == 0)(lambda: await_rows(2 * members - 2))
        pl.when(g > 0)(lambda: await_rows(2 * members))
        rows = received[pl.ds(pl.multiple_of(2 * members * g, 2 * members), 2 * members), :]
        rows = jnp.transpose(jnp.concatenate([rows, rows], axis=0))
        values = [jnp.where(low_half, rows[16 * v : 16 * v + 8], rows[16 * v + 8 : 16 * v + 16]) for v in range(8)]
        for v in range(4):
            places[0, g, v * ranks : (v + 1) * ranks, :] = values[v]
        share(places, place_send, place_recv, g)

        for j in range(ranks // 2):
            pair = jnp.concatenate(
                [one_hot(values[0][r : r + 1], elements) for r in (2 * j, 2 * j + 1)], axis=1
            )
            taken = jnp.dot(coef[...], pair, preferred_element_type=F32)
            taken = taken[:HALF] + taken[HALF:]
            for side in range(2):
                at = (2 * j + side) * PITCH
                strided[at : at + HALF, :] = taken[:, side * LANES : (side + 1) * LANES]
        first, second, third = basis(values[1]), basis(values[2]), basis(values[3])
        plane = [x * y for x in second for y in third]
        for c in range(3):
            speed = None
            for a in range(3):
                inner = None
                for k in range(9):
                    term = plane[k] * strided[pl.ds(c * 27 + a * 9 + k, ranks, stride=PITCH), :]
                    inner = term if inner is None else inner + term
                inner = first[a] * inner
                speed = inner if speed is None else speed + inner
            forces[0, g, c * ranks : (c + 1) * ranks, :] = values[7] * (values[4 + c] - speed)
        share(forces, force_send, force_recv, g)

        for c in range(3):
            lower = tile(forces, 0, g, c)
            turned[c * 16 : c * 16 + 8, :] = lower
            turned[c * 16 + 8 : c * 16 + 16, :] = pltpu.roll(lower, LANES // 2, 1)
        flipped[...] = jnp.transpose(turned[...])[: 2 * members, :]
        even = flipped[pl.ds(0, members, stride=2), :]
        odd = flipped[pl.ds(1, members, stride=2), :]
        base = pl.multiple_of(g * members, members)
        answer[pl.ds(base, members), :] = jnp.where(low_rows, even, pltpu.roll(odd, LANES // 2, 1))
        for j in range(members - 1, -1, -1):
            steps = g * (members // 2) + (j + 1) // 2
            partner = lax.rem(me + (owners - steps if j % 2 else steps), owners)

            def reply(j=j, partner=partner):
                row = pl.ds(base + j, 1)
                pltpu.make_async_remote_copy(
                    src_ref=answer.at[row, :], dst_ref=returned.at[row, :], send_sem=back_sem.at[0],
                    recv_sem=back_sem.at[1], device_id=(partner, leaf), device_id_type=MESH,
                ).start()

            if j:
                reply()
            else:
                pl.when(g > 0)(reply)
        pl.when(order == 0)(contact)
        return carry

    corner = leaf.astype(F32) * float(per_leaf)

    def scatter(g):
        added = None
        for source in range(peers):
            first, second, third = (basis(tile(places, source, g, v)) for v in (1, 2, 3))
            plane = [x * y for x in second for y in third]
            half = source % 2 * (ranks * PITCH)
            for c in range(3):
                for a in range(3):
                    scaled = tile(forces, source, g, c) * first[a]
                    for k in range(9):
                        strided[pl.ds(half + c * 27 + a * 9 + k, ranks, stride=PITCH), :] = scaled * plane[k]
            near = tile(places, source, g, 0) - corner
            terms, hots = [], []
            for r in range(ranks):
                at = half + r * PITCH
                terms.append(jnp.concatenate(split(strided[at : at + HALF, :]), axis=0))
                hots.append(one_hot(near[r : r + 1], per_leaf))
            part = lax.dot_general(
                jnp.concatenate(hots, axis=1), jnp.concatenate(terms, axis=1), NT, preferred_element_type=F32
            )
            added = part if added is None else added + part
        total[:, : 2 * HALF] += added

    total[...] = jnp.zeros_like(total)
    turned[...] = jnp.zeros_like(turned)
    lax.fori_loop(0, GROUPS, gather, 0)
    returned[0:1, :] = answer[0:1, :]
    strided[...] = jnp.zeros_like(strided)

    def gathered(i, carry):
        g = turn(i)
        arrived(places, place_send, place_recv, g)
        arrived(forces, force_send, force_recv, g)
        scatter(g)
        return carry

    lax.fori_loop(0, GROUPS, gathered, 0)
    sums = jnp.transpose(total[...])
    flow_out[...] = sums[:81] + sums[HALF : HALF + 81]

    pltpu.make_async_remote_copy(
        src_ref=patch_part.at[: peers - 1], dst_ref=patch_all.at[: peers - 1], send_sem=patch_sem.at[0],
        recv_sem=patch_sem.at[1], device_id=(me, leaf_peer(1)), device_id_type=MESH,
    ).wait()
    patch_out[...] = (patch_all[0] + patch_all[1]) + (patch_all[2] + patch_all[3])

    pltpu.make_async_remote_copy(
        src_ref=answer.at[: owners - 1, :], dst_ref=returned.at[: owners - 1, :], send_sem=back_sem.at[0],
        recv_sem=back_sem.at[1], device_id=(ahead_of(1), leaf), device_id_type=MESH,
    ).wait()
    high, low = split(jnp.transpose(returned[...]))
    twice = jnp.concatenate([dest_hot[...], dest_hot[...]], axis=0)
    at_owner = jnp.dot(jnp.concatenate([high, low], axis=1), twice, preferred_element_type=F32)
    number = lax.broadcasted_iota(jnp.int32, (16, points), 0).astype(F32)
    for c in range(3):
        fsi = jnp.zeros((1, points), F32)
        for h in range(2):
            at = h * (LANES // 2) + c * 16
            mine = number == rank_row[...] - float(16 * h)
            fsi = fsi + jnp.sum(jnp.where(mine, at_owner[at : at + 16], 0.0), axis=0, keepdims=True)
        shell_out[c : c + 1, :] = push[c : c + 1, :] - fsi

    pltpu.make_async_remote_copy(
        src_ref=message.at[: 2 * (owners - 1), :], dst_ref=received.at[: 2 * (owners - 1), :], send_sem=out_send,
        recv_sem=out_recv.at[0], device_id=(ahead_of(1), leaf), device_id_type=MESH,
    ).wait_send()
    for buffer, send, recv in ((places, place_send, place_recv), (forces, force_send, force_recv)):
        pltpu.make_async_remote_copy(
            src_ref=buffer.at[1:], dst_ref=buffer.at[1:], send_sem=send, recv_sem=recv.at[0],
            device_id=(me, leaf_peer(1)), device_id_type=MESH,
        ).wait_send()


def finish(flow_in, shell_in, patch_in, flow_out, shell_out, patch_out, sems):
    copies = [
        pltpu.make_async_copy(src, dst, sems.at[i])
        for i, (src, dst) in enumerate(((flow_in, flow_out), (shell_in, shell_out), (patch_in, patch_out)))
    ]
    for copy in copies:
        copy.start()
    for copy in copies:
        copy.wait()


def solution(mesh):
    owners, peers = mesh.shape["flow"], mesh.shape["leaf"]

    def per_device(
        vel_coef, gp_block, gp_elem, gp_param, gp_vel, gp_weight, gp_pos, contact_patch, contact_param, patch_ctrl
    ):
        points, elements, patches = gp_elem.shape[0], vel_coef.shape[1], patch_ctrl.shape[1]
        per_leaf = elements // peers
        ranks = CAP * owners // GROUPS // LANES
        vmem = pl.BlockSpec(memory_space=pltpu.VMEM)
        outs = (
            jax.ShapeDtypeStruct((81, per_leaf), F32),
            jax.ShapeDtypeStruct((3, points), F32),
            jax.ShapeDtypeStruct((27, patches), F32),
        )
        arguments = (
            vel_coef,
            gp_block.reshape(1, points),
            gp_elem.reshape(1, points),
            gp_param,
            gp_vel,
            gp_weight.reshape(1, points),
            gp_pos,
            contact_patch.reshape(1, points),
            contact_param,
            patch_ctrl,
        )
        results = pl.pallas_call(
            kernel,
            out_shape=tuple(pltpu.VMEM(x.shape, x.dtype) for x in outs),
            in_specs=[pl.BlockSpec(memory_space=pl.ANY)] * 10,
            out_specs=(vmem,) * 3,
            scratch_shapes=[pltpu.VMEM(x.shape, x.dtype) for x in arguments]
            + [
                pltpu.VMEM((owners, points), BF16),
                pltpu.VMEM((1, points), F32),
                pltpu.VMEM((4 * LANES, points), BF16),
                pltpu.VMEM((2 * owners, LANES), F32),
                pltpu.VMEM((2 * owners, LANES), F32),
                pltpu.VMEM((peers, GROUPS, 4 * ranks, LANES), F32),
                pltpu.VMEM((2 * HALF, elements), BF16),
                pltpu.VMEM((peers, GROUPS, 3 * ranks, LANES), F32),
                pltpu.VMEM((LANES, LANES), F32),
                pltpu.VMEM((2 * owners // GROUPS, LANES), F32),
                pltpu.VMEM((owners, LANES), F32),
                pltpu.VMEM((owners, LANES), F32),
                pltpu.VMEM((2 * ranks * PITCH, LANES), F32),
                pltpu.VMEM((per_leaf, 2 * LANES), F32),
                pltpu.VMEM((LANES, points), BF16),
                pltpu.VMEM((3, points), F32),
                pltpu.VMEM((peers, 27, patches), F32),
                pltpu.VMEM((peers, 27, patches), F32),
                pltpu.VMEM((peers, 27, patches), F32),
                pltpu.SemaphoreType.DMA((10,)),
                pltpu.SemaphoreType.DMA,
                pltpu.SemaphoreType.DMA((GROUPS,)),
                pltpu.SemaphoreType.DMA((2,)),
                pltpu.SemaphoreType.DMA((2,)),
                pltpu.SemaphoreType.DMA((2,)),
                pltpu.SemaphoreType.DMA,
                pltpu.SemaphoreType.DMA((GROUPS,)),
                pltpu.SemaphoreType.DMA,
                pltpu.SemaphoreType.DMA((GROUPS,)),
            ],
            compiler_params=pltpu.CompilerParams(
                collective_id=0, has_side_effects=True, vmem_limit_bytes=60 * 1024 * 1024
            ),
        )(*arguments)
        return pl.pallas_call(
            finish,
            out_shape=outs,
            in_specs=[vmem] * 3,
            out_specs=(pl.BlockSpec(memory_space=pl.ANY),) * 3,
            scratch_shapes=[pltpu.SemaphoreType.DMA((3,))],
        )(
            *[pltpu.with_memory_space_constraint(x, pltpu.VMEM) for x in results]
        )

    both = ("flow", "leaf")
    return jax.shard_map(
        per_device,
        mesh=mesh,
        in_specs=(
            P(None, "flow"), P(both, None), P(both), P(None, both), P(None, both),
            P(both), P(None, both), P(both), P(None, both), P(None, both),
        ),
        out_specs=(P(None, both), P(None, both), P(None, both)),
        check_vma=False,
    )
```
